32 devices in a mesh: lon: 8 (over z, x), lat: 4 (over y, core).
Axes of the slice: x: 2, y: 2, z: 4, core: 2. Of those that a mesh axis runs over, the one named last changes fastest.
Arguments:
- state: float32 [2048, 64, 1024], P('lon', None, 'lat'), may hold values from -6 to 6
Outputs:
- spectrum: float32 [2, 1024, 64, 1024], P(None, 'lon', None, 'lat')
The draws below stay inside these ranges and needn't reach their ends.
All inputs are finite; a program needn't handle non-finite values.
Results may differ from the reference program's by a relative error of at most 0.00011.
Values sent between devices are 32-bit elements; how exact they have to be, the bound alone decides.
A program may use at most 128 MiB of HBM per device.

```python
import math
import jax
import jax.numpy as jnp

NLON = 2048
FIELDS = 64
NLAT = 1024
MODES = 1024


def steps_of(rng, shape, pieces, least, top_value):
    loudness = 1.0
    for dim, blocks in pieces:
        draws = jax.random.uniform(jax.random.fold_in(jax.random.fold_in(rng, 6), dim), (blocks,), jnp.float32, least / len(pieces), top_value / len(pieces))
        loudness = loudness * jnp.repeat(jnp.exp(draws), shape[dim] // blocks).reshape((-1,) + (1,) * (len(shape) - 1 - dim))
    return loudness


def noise(rng, dims, deviation, limit, shards=(), kind=jnp.bfloat16):
    array = jax.random.normal(rng, dims, jnp.float32) * deviation
    if len(shards) > 0:
        array = steps_of(rng, dims, shards, -0.22, 0.18) * array
    return jnp.clip(array, min=-limit, max=limit).astype(kind)


def setup_inputs(seed: int = 0) -> dict:
    arg_keys = jax.random.split(jax.random.key(seed), 2)
    return {
        "state": noise(arg_keys[0], (NLON, FIELDS, NLAT), 1.0, 6.0, ((0, 8), (2, 4)), jnp.float32),
    }


def reference(state):
    spectrum = jnp.fft.rfft(state, axis=0)[:MODES] * (1.0 / math.sqrt(NLON))
    return jnp.stack([jnp.real(spectrum), jnp.imag(spectrum)]).astype(jnp.float32)
```

```python
import functools
import math

import jax
import jax.numpy as jnp
import numpy as np
from jax import lax
from jax.experimental import pallas as pl
from jax.experimental.pallas import tpu as pltpu
from jax.sharding import PartitionSpec as P

RADIX = 8
LANES = 128
SUBLANES = 8
TILE = 16
SIDE = RADIX // 2
PAIRS = SUBLANES // 2
EXTRA = 24
LAG = 5
GRID_SLOTS = 7
OTHER_SLOTS = 3
CODED_SLOTS = 3
ARRIVED_SLOTS = 4
DONE_SLOTS = 7
CROSS_SLOTS = 4
VMEM_LIMIT = 46 * 1024 * 1024


def phase_angle(first_index, second_index, period):
    product = first_index * second_index % period
    return product.astype(jnp.float32) * (2.0 * math.pi / period)


def dense_spectrum(gathered, factor):
    lon_count = gathered.shape[0]
    mode_count = lon_count // 2
    wavenum = lax.broadcasted_iota(jnp.int32, (mode_count, lon_count), 0)
    longitude = lax.broadcasted_iota(jnp.int32, (mode_count, lon_count), 1)
    angles = phase_angle(wavenum, longitude, lon_count)
    real_part = jnp.dot(
        jnp.cos(angles) * factor,
        gathered,
        precision=lax.Precision.HIGHEST,
        preferred_element_type=jnp.float32,
    )
    imag_part = jnp.dot(
        -jnp.sin(angles) * factor,
        gathered,
        precision=lax.Precision.HIGHEST,
        preferred_element_type=jnp.float32,
    )
    return jnp.stack([real_part, imag_part])


def dense_local(state):
    lon_dev, fields, lat_dev = state.shape
    devices = lax.axis_size("lon")
    columns = state.reshape(lon_dev, fields * lat_dev)
    factor = 1.0 / math.sqrt(lon_dev * devices)
    gathered = lax.all_to_all(columns, "lon", split_axis=1, concat_axis=0, tiled=True)
    spectrum = dense_spectrum(gathered, factor)
    shares = lax.all_to_all(spectrum, "lon", split_axis=1, concat_axis=2, tiled=True)
    return shares.reshape(2, shares.shape[1], fields, lat_dev)


def split(value):
    high = value.astype(jnp.bfloat16)
    return high, (value - high.astype(jnp.float32)).astype(jnp.bfloat16)


def split_table(table):
    high = table.astype(jnp.bfloat16)
    return high, (table - high.astype(np.float64)).astype(jnp.bfloat16)


def dft_rows(wavenums, places, count):
    angle = 2.0 * np.pi / count * (wavenums[:, None] * places[None] % count)
    scale = 1.0 / math.sqrt(count)
    return scale * np.cos(angle), -scale * np.sin(angle)


def by_owner(parts):
    shaped = [part.reshape(SIDE, -1, part.shape[1]) for part in parts]
    return np.stack(shaped, 1).reshape(-1, parts[0].shape[1])


def side_tables(points, side):
    count, band = RADIX * points, RADIX * points // 4
    places = side * (count // 2) + np.arange(count // 2)
    step = 2 * np.arange(band // 2)

    def rows(first):
        return by_owner(dft_rows(first + step, places, count))

    own = [rows(side * band + parity).reshape(SIDE, 1, -1, count // 2) for parity in range(2)]
    own = np.concatenate(own, 1).reshape(2 * band, count // 2)
    even, odd = rows((1 - side) * band), rows((1 - side) * band + 1)
    power = (even * even).sum(1)
    spread = (odd @ even.T) * np.where(power > 1e-9, 1.0 / np.maximum(power, 1e-9), 0.0)
    left = odd - spread @ even
    picked, columns = [], []
    for _ in range(EXTRA):
        row, column = np.unravel_index(np.argmax(np.abs(left)), left.shape)
        picked.append(row)
        columns.append(left[:, column] / left[row, column])
        left = left - np.outer(columns[-1], left[row])
    columns = np.stack(columns, 1)
    mix = np.linalg.solve(columns[picked].T, columns.T).T
    rank, padded = band + EXTRA, -(-(band + EXTRA) // 16) * 16
    sent = np.zeros((padded, count // 2))
    sent[:rank] = np.concatenate([even, odd[picked]])
    fill = np.zeros((band, padded))
    fill[:, :rank] = np.concatenate([spread - mix @ spread[picked], mix], 1)
    return own, sent, fill


def all_tables(points):
    sides = [side_tables(points, side) for side in range(2)]
    out = []
    for tables in zip(*sides):
        for piece in split_table(np.stack(tables)):
            out.append(jnp.asarray(piece))
    return out


def kernel(
    chunks, rank,
    state, own_hi_all, own_lo_all, sent_hi_all, sent_lo_all, fill_hi_all, fill_lo_all, out,
    inb, grid, other, coded, arrived, done, cross,
    own_hi, own_lo, sent_hi, sent_lo, fill_hi, fill_lo, x_hi, x_lo, c_hi, c_lo,
    in_sem, table_sem, xs_send, xs_recv, zs_send, zs_recv, m_send, m_recv,
    zo_send, zo_recv, xo_send, xo_recv,
):
    points = state.shape[0]
    modes = points // 2
    groups = chunks // PAIRS
    padded = coded.shape[1]
    me = lax.axis_index("lon")
    z, x = me // 2, lax.rem(me, 2)
    row, side = lax.rem(z, 2), z // 2
    place = lax.rem(me, SIDE)
    beside = place + 1 - 2 * x
    inner = lax.rem((z + 1) // 2, 2) == 1
    outer = lax.rem((z + 1) // 2, 2) == 0
    x_peer = me + 1 - 2 * x
    z_peer = me + 2 - 4 * row
    m_peer = (3 - z) * 2 + x

    def remote(source, target, send, recv, peer):
        return pltpu.make_async_remote_copy(
            src_ref=source, dst_ref=target, send_sem=send, recv_sem=recv,
            device_id={"lon": peer}, device_id_type=pl.DeviceIdType.MESH,
        )

    def load(group, half):
        slot = lax.rem(group, 2)
        fields = pl.ds(pl.multiple_of(group * SUBLANES, SUBLANES), SUBLANES)
        return pltpu.make_async_copy(
            state.at[:, fields, half * LANES : (half + 1) * LANES],
            inb.at[slot, half], in_sem.at[slot, half],
        )

    def samples_x(t, target_place):
        slot = lax.rem(t, GRID_SLOTS)
        return remote(
            other.at[lax.rem(t, OTHER_SLOTS)], grid.at[slot, target_place],
            xs_send.at[lax.rem(t, OTHER_SLOTS)], xs_recv.at[slot], x_peer,
        )

    def samples_z(t, which, line):
        slot = lax.rem(t, GRID_SLOTS)
        ref = grid.at[slot, line * 2 + which]
        return remote(ref, ref, zs_send.at[slot, which], zs_recv.at[slot, which], z_peer)

    def code(t):
        rows = pl.ds(0, rank)
        here, there = lax.rem(t, CODED_SLOTS), lax.rem(t, ARRIVED_SLOTS)
        return remote(
            coded.at[here, rows], arrived.at[there, rows], m_send.at[here], m_recv.at[there], m_peer
        )

    def modes_z(t, which, line):
        slot = lax.rem(t, DONE_SLOTS)
        ref = done.at[slot, line * 2 + which]
        return remote(ref, ref, zo_send.at[slot, which], zo_recv.at[slot, which], z_peer)

    def modes_x(t):
        slot, there = lax.rem(t, DONE_SLOTS), lax.rem(t, CROSS_SLOTS)
        return remote(
            done.at[slot, beside], cross.at[there], xo_send.at[slot], xo_recv.at[there], x_peer
        )

    tables = [
        pltpu.make_async_copy(source.at[which], target, table_sem.at[index])
        for index, (source, which, target) in enumerate((
            (sent_hi_all, side, sent_hi), (sent_lo_all, side, sent_lo),
            (own_hi_all, side, own_hi), (own_lo_all, side, own_lo),
            (fill_hi_all, 1 - side, fill_hi), (fill_lo_all, 1 - side, fill_lo),
        ))
    ]
    in_rows = inb.reshape(2 * 2 * points * SUBLANES, LANES)
    out_rows = out.reshape(2 * modes * groups * 2 * SUBLANES, LANES)
    k_rows = groups * 2 * SUBLANES

    def arrange(t):
        group, pair = t // PAIRS, lax.rem(t, PAIRS)

        @pl.when(pair == 0)
        def _():
            for half in range(2):
                load(group, half).wait()

        @pl.when(t >= OTHER_SLOTS)
        def _():
            samples_x(t - OTHER_SLOTS, place).wait_send()

        slot, spare = lax.rem(t, GRID_SLOTS), lax.rem(t, OTHER_SLOTS)

        def tile(index, carry):
            first = pl.multiple_of(index * TILE, TILE)
            for field in range(2):
                lanes = pl.ds(field * LANES, LANES)

                def read(half):
                    base = ((lax.rem(group, 2) * 2 + half) * points + first) * SUBLANES
                    return in_rows[pl.ds(base + 2 * pair + field, TILE, stride=SUBLANES), :]

                other[spare, pl.ds(first, TILE), lanes] = read(1 - x)
                grid[slot, place, pl.ds(first, TILE), lanes] = read(x)
            return carry

        lax.fori_loop(0, points // TILE, tile, 0)

        @pl.when((pair == PAIRS - 1) & (group + 2 < groups))
        def _():
            for half in range(2):
                load(group + 2, half).start()

        samples_x(t, place).start()

    def store(t, half, ref):
        group, pair = t // PAIRS, lax.rem(t, PAIRS)
        share = modes // 2
        for parity in range(2):
            for part in range(2):
                for field in range(2):
                    first = (part * modes + parity) * k_rows
                    base = first + (group * 2 + half) * SUBLANES + 2 * pair + field
                    out_rows[pl.ds(base, share, stride=2 * k_rows), :] = ref[
                        pl.ds((parity * 2 + part) * share, share), pl.ds(field * LANES, LANES)
                    ]

    def dot3(a_hi, a_lo, b_hi, b_lo):
        dot = functools.partial(jnp.dot, preferred_element_type=jnp.float32)
        return dot(a_hi, b_hi) + dot(a_hi, b_lo) + dot(a_lo, b_hi)

    def encode(t):
        slot, here = lax.rem(t, GRID_SLOTS), lax.rem(t, CODED_SLOTS)
        for which in range(SIDE):

            def tile(index, carry):
                first = pl.multiple_of(index * 32, 32)
                high, low = split(grid[slot, which, pl.ds(first, 32), :])
                rows = pl.ds(pl.multiple_of(which * points + first, 32), 32)
                x_hi[rows, :] = high
                x_lo[rows, :] = low
                return carry

            lax.fori_loop(0, points // 32, tile, 0)

        @pl.when(t >= CODED_SLOTS)
        def _():
            code(t - CODED_SLOTS).wait_send()

        coded[here] = dot3(sent_hi[...], sent_lo[...], x_hi[...], x_lo[...])
        code(t).start()

    def own_modes(t):
        slot = lax.rem(t, DONE_SLOTS)

        @pl.when(t >= DONE_SLOTS)
        def _():
            for which in range(2):
                modes_z(t - DONE_SLOTS, which, 1 - row).wait_send()
            modes_x(t - DONE_SLOTS).wait_send()

        def block(which, carry):
            rows = pl.ds(pl.multiple_of(which * points, points), points)
            done[slot, which] = dot3(own_hi[rows, :], own_lo[rows, :], x_hi[...], x_lo[...])
            return carry

        lax.fori_loop(0, SIDE, block, 0)

    def decode(t):
        slot, there = lax.rem(t, DONE_SLOTS), lax.rem(t, ARRIVED_SLOTS)

        def tile(index, carry):
            rows = pl.ds(pl.multiple_of(index * 32, 32), 32)
            high, low = split(arrived[there, rows, :])
            c_hi[rows, :] = high
            c_lo[rows, :] = low
            return carry

        lax.fori_loop(0, padded // 32, tile, 0)
        odd = dot3(fill_hi[...], fill_lo[...], c_hi[...], c_lo[...])
        share = modes
        for which in range(SIDE):
            rows = slice(which * share, (which + 1) * share)
            done[slot, which, :share] += arrived[there, rows]
            done[slot, which, share:] += odd[rows]

    for group in range(2):
        for half in range(2):
            load(group, half).start()

    @pl.when(inner)
    def _():
        for copy in tables:
            copy.start()

    arrived[:, rank:padded] = jnp.zeros((arrived.shape[0], padded - rank, arrived.shape[2]), jnp.float32)
    barrier = pltpu.get_barrier_semaphore()
    for peer in (x_peer, z_peer, m_peer):
        pl.semaphore_signal(
            barrier, inc=1, device_id={"lon": peer}, device_id_type=pl.DeviceIdType.MESH
        )
    pl.semaphore_wait(barrier, 3)

    arrange(0)

    @pl.when(outer)
    def _():
        samples_z(0, x, row).start()

    def step(i, carry):
        @pl.when(outer & (i >= 2) & (i < chunks + 2))
        def _():
            for which in range(2):
                samples_z(i - 2, which, row).wait_send()

        @pl.when(i + 1 < chunks)
        def _():
            arrange(i + 1)

        @pl.when(i < chunks)
        def _():
            samples_x(i, beside).wait_recv()

        @pl.when(outer & (i < chunks))
        def _():
            samples_z(i, 1 - x, row).start()

            @pl.when(i + 1 < chunks)
            def _():
                samples_z(i + 1, x, row).start()

        @pl.when(outer & (i >= LAG) & (i < chunks + LAG))
        def _():
            t = i - LAG
            modes_z(t, 1 - x, row).wait_recv()
            modes_x(t).start()
            modes_z(t, x, row).wait_recv()
            store(t, x, done.at[lax.rem(t, DONE_SLOTS), place])

        @pl.when(outer & (i >= LAG + 1) & (i < chunks + LAG + 1))
        def _():
            t = i - LAG - 1
            modes_x(t).wait_send()
            modes_x(t).wait_recv()
            store(t, 1 - x, cross.at[lax.rem(t, CROSS_SLOTS)])

        @pl.when(inner & (i < chunks))
        def _():
            for which in range(2):
                samples_z(i, which, 1 - row).wait_recv()

            @pl.when(i == 0)
            def _():
                for copy in tables:
                    copy.wait()

            encode(i)
            own_modes(i)

        @pl.when(inner & (i >= 1) & (i < chunks + 1))
        def _():
            t = i - 1
            code(t).wait_recv()
            decode(t)
            modes_z(t, 1 - x, 1 - row).start()
            modes_x(t).start()
            modes_z(t, x, 1 - row).start()
            store(t, x, done.at[lax.rem(t, DONE_SLOTS), place])

        @pl.when(inner & (i >= 2) & (i < chunks + 2))
        def _():
            t = i - 2
            modes_x(t).wait_recv()
            store(t, 1 - x, cross.at[lax.rem(t, CROSS_SLOTS)])

        return carry

    lax.fori_loop(0, chunks + LAG + 1, step, 0)

    for back in range(OTHER_SLOTS):
        samples_x(chunks - 1 - back, place).wait_send()

    @pl.when(inner)
    def _():
        for back in range(CODED_SLOTS):
            code(chunks - 1 - back).wait_send()
        for back in range(DONE_SLOTS):
            for which in range(2):
                modes_z(chunks - 1 - back, which, 1 - row).wait_send()
            modes_x(chunks - 1 - back).wait_send()


def fused_local(state):
    points, fields, lat_dev = state.shape
    modes = points // 2
    groups = fields // SUBLANES
    chunks = groups * PAIRS
    tables = all_tables(points)
    padded = tables[2].shape[1]
    rank = RADIX * points // 4 + EXTRA
    vmem = pl.BlockSpec(memory_space=pltpu.VMEM)
    hbm = pl.BlockSpec(memory_space=pl.ANY)
    wide = 2 * LANES
    dma = pltpu.SemaphoreType.DMA

    def f32(*shape):
        return pltpu.VMEM(shape, jnp.float32)

    def bf16(*shape):
        return pltpu.VMEM(shape, jnp.bfloat16)

    result = pl.pallas_call(
        functools.partial(kernel, chunks, rank),
        out_shape=pltpu.VMEM((2, modes, groups, 2, SUBLANES, LANES), jnp.float32),
        in_specs=[hbm] * (1 + len(tables)),
        out_specs=vmem,
        scratch_shapes=[
            f32(2, 2, points, SUBLANES, LANES),
            f32(GRID_SLOTS, SIDE, points, wide),
            f32(OTHER_SLOTS, points, wide),
            f32(CODED_SLOTS, padded, wide),
            f32(ARRIVED_SLOTS, padded, wide),
            f32(DONE_SLOTS, SIDE, points, wide),
            f32(CROSS_SLOTS, points, wide),
            *[bf16(*table.shape[1:]) for table in tables],
            bf16(SIDE * points, wide),
            bf16(SIDE * points, wide),
            bf16(padded, wide),
            bf16(padded, wide),
            dma((2, 2)),
            dma((len(tables),)),
            dma((OTHER_SLOTS,)),
            dma((GRID_SLOTS,)),
            dma((GRID_SLOTS, 2)),
            dma((GRID_SLOTS, 2)),
            dma((CODED_SLOTS,)),
            dma((ARRIVED_SLOTS,)),
            dma((DONE_SLOTS, 2)),
            dma((DONE_SLOTS, 2)),
            dma((DONE_SLOTS,)),
            dma((CROSS_SLOTS,)),
        ],
        compiler_params=pltpu.CompilerParams(
            collective_id=0, has_side_effects=True, vmem_limit_bytes=VMEM_LIMIT
        ),
    )(state, *tables)
    return result.transpose(0, 1, 2, 4, 3, 5).reshape(2, modes, fields, lat_dev)


def solution(mesh):
    devices = mesh.shape["lon"]

    def local(state):
        points, fields, lat_dev = state.shape
        fits = (
            devices == RADIX
            and fields == RADIX * SUBLANES
            and points == 2 * LANES
            and lat_dev == 2 * LANES
        )
        return fused_local(state) if fits else dense_local(state)

    return jax.shard_map(
        local,
        mesh=mesh,
        in_specs=(P("lon", None, "lat"),),
        out_specs=P(None, "lon", None, "lat"),
        check_vma=False,
    )
```

```python
import functools
import math

import jax
import jax.numpy as jnp
import numpy as np
from jax import lax
from jax.experimental import pallas as pl
from jax.experimental.pallas import tpu as pltpu
from jax.sharding import PartitionSpec as P

RADIX = 8
LANES = 128
SUBLANES = 8
TILE = 16
SIDE = RADIX // 2
FIELDS = 1
PIECES = SUBLANES // FIELDS
AHEAD = 2
SENT_LAG = 2
EXTRA = 24
LAG = 7
GRID_SLOTS = 9
OTHER_SLOTS = 4
CODED_SLOTS = 3
ARRIVED_SLOTS = 4
DONE_SLOTS = 9
CROSS_SLOTS = 5
VMEM_LIMIT = 46 * 1024 * 1024


def phase_angle(first_index, second_index, period):
    product = first_index * second_index % period
    return product.astype(jnp.float32) * (2.0 * math.pi / period)


def dense_spectrum(gathered, factor):
    lon_count = gathered.shape[0]
    mode_count = lon_count // 2
    wavenum = lax.broadcasted_iota(jnp.int32, (mode_count, lon_count), 0)
    longitude = lax.broadcasted_iota(jnp.int32, (mode_count, lon_count), 1)
    angles = phase_angle(wavenum, longitude, lon_count)
    real_part = jnp.dot(
        jnp.cos(angles) * factor,
        gathered,
        precision=lax.Precision.HIGHEST,
        preferred_element_type=jnp.float32,
    )
    imag_part = jnp.dot(
        -jnp.sin(angles) * factor,
        gathered,
        precision=lax.Precision.HIGHEST,
        preferred_element_type=jnp.float32,
    )
    return jnp.stack([real_part, imag_part])


def dense_local(state):
    lon_dev, fields, lat_dev = state.shape
    devices = lax.axis_size("lon")
    columns = state.reshape(lon_dev, fields * lat_dev)
    factor = 1.0 / math.sqrt(lon_dev * devices)
    gathered = lax.all_to_all(columns, "lon", split_axis=1, concat_axis=0, tiled=True)
    spectrum = dense_spectrum(gathered, factor)
    shares = lax.all_to_all(spectrum, "lon", split_axis=1, concat_axis=2, tiled=True)
    return shares.reshape(2, shares.shape[1], fields, lat_dev)


def split(value):
    high = value.astype(jnp.bfloat16)
    return high, (value - high.astype(jnp.float32)).astype(jnp.bfloat16)


def split_table(table):
    high = table.astype(jnp.bfloat16)
    return high, (table - high.astype(np.float64)).astype(jnp.bfloat16)


def dft_rows(wavenums, places, count):
    angle = 2.0 * np.pi / count * (wavenums[:, None] * places[None] % count)
    scale = 1.0 / math.sqrt(count)
    return scale * np.cos(angle), -scale * np.sin(angle)


def by_owner(parts):
    shaped = [part.reshape(SIDE, -1, part.shape[1]) for part in parts]
    return np.stack(shaped, 1).reshape(-1, parts[0].shape[1])


def side_tables(points, side):
    count, band = RADIX * points, RADIX * points // 4
    places = side * (count // 2) + np.arange(count // 2)
    step = 2 * np.arange(band // 2)

    def rows(first):
        return by_owner(dft_rows(first + step, places, count))

    own = [rows(side * band + parity).reshape(SIDE, 1, -1, count // 2) for parity in range(2)]
    own = np.concatenate(own, 1).reshape(2 * band, count // 2)
    even, odd = rows((1 - side) * band), rows((1 - side) * band + 1)
    power = (even * even).sum(1)
    spread = (odd @ even.T) * np.where(power > 1e-9, 1.0 / np.maximum(power, 1e-9), 0.0)
    left = odd - spread @ even
    picked, columns = [], []
    for _ in range(EXTRA):
        row, column = np.unravel_index(np.argmax(np.abs(left)), left.shape)
        picked.append(row)
        columns.append(left[:, column] / left[row, column])
        left = left - np.outer(columns[-1], left[row])
    columns = np.stack(columns, 1)
    mix = np.linalg.solve(columns[picked].T, columns.T).T
    rank, padded = band + EXTRA, -(-(band + EXTRA) // 16) * 16
    sent = np.zeros((padded, count // 2))
    sent[:rank] = np.concatenate([even[: band // 2], odd[picked], even[band // 2 :]])
    fill = np.zeros((band, padded))
    spread = spread - mix @ spread[picked]
    fill[:, :rank] = np.concatenate([spread[:, : band // 2], mix, spread[:, band // 2 :]], 1)
    return own, sent, fill


def all_tables(points):
    sides = [side_tables(points, side) for side in range(2)]
    out = []
    for tables in zip(*sides):
        for piece in split_table(np.stack(tables)):
            out.append(jnp.asarray(piece))
    return out


def kernel(
    chunks, rank,
    state, own_hi_all, own_lo_all, sent_hi_all, sent_lo_all, fill_hi_all, fill_lo_all, out,
    inb, grid, other, coded, arrived, done, cross,
    own_hi, own_lo, sent_hi, sent_lo, fill_hi, fill_lo, x_hi, x_lo, c_hi, c_lo,
    in_sem, table_sem, xs_send, xs_recv, zs_send, zs_recv, m_send, m_recv,
    zo_send, zo_recv, xo_send, xo_recv,
):
    points = state.shape[0]
    modes = points // 2
    groups = chunks // PIECES
    padded, band = coded.shape[1], rank - EXTRA
    me = lax.axis_index("lon")
    z, x = me // 2, lax.rem(me, 2)
    row, side = lax.rem(z, 2), z // 2
    place = lax.rem(me, SIDE)
    beside = place + 1 - 2 * x
    inner = lax.rem((z + 1) // 2, 2) == 1
    outer = lax.rem((z + 1) // 2, 2) == 0
    x_peer = me + 1 - 2 * x
    z_peer = me + 2 - 4 * row
    m_peer = (3 - z) * 2 + x

    def remote(source, target, send, recv, peer):
        return pltpu.make_async_remote_copy(
            src_ref=source, dst_ref=target, send_sem=send, recv_sem=recv,
            device_id={"lon": peer}, device_id_type=pl.DeviceIdType.MESH,
        )

    def load(group, half):
        slot = lax.rem(group, 2)
        fields = pl.ds(pl.multiple_of(group * SUBLANES, SUBLANES), SUBLANES)
        return pltpu.make_async_copy(
            state.at[:, fields, half * LANES : (half + 1) * LANES],
            inb.at[slot, half], in_sem.at[slot, half],
        )

    def cut(part):
        return pl.ds(part * modes, modes)

    def samples_x(t, target_place, part):
        here, slot = lax.rem(t, OTHER_SLOTS), lax.rem(t, GRID_SLOTS)
        return remote(
            other.at[here, cut(part)], grid.at[slot, target_place, cut(part)],
            xs_send.at[here, part], xs_recv.at[slot, part], x_peer,
        )

    def samples_z(t, which, line, part):
        slot = lax.rem(t, GRID_SLOTS)
        ref = grid.at[slot, line * 2 + which, cut(part)]
        return remote(ref, ref, zs_send.at[slot, which, part], zs_recv.at[slot, which, part], z_peer)

    def evens(line):
        return line * (band // 2 + EXTRA)

    def code(t, part, line):
        if part == 0:
            rows = pl.ds(evens(line), band // 2)
        else:
            rows = pl.ds((1 - line) * (band // 2), band // 2 + EXTRA)
        here, there = lax.rem(t, CODED_SLOTS), lax.rem(t, ARRIVED_SLOTS)
        return remote(
            coded.at[here, rows], arrived.at[there, rows],
            m_send.at[here, part], m_recv.at[there, part], m_peer,
        )

    def modes_z(t, which, line, part):
        slot = lax.rem(t, DONE_SLOTS)
        ref = done.at[slot, line * 2 + which, cut(part)]
        return remote(ref, ref, zo_send.at[slot, which, part], zo_recv.at[slot, which, part], z_peer)

    def modes_x(t, part):
        slot, there = lax.rem(t, DONE_SLOTS), lax.rem(t, CROSS_SLOTS)
        return remote(
            done.at[slot, beside, cut(part)], cross.at[there, cut(part)],
            xo_send.at[slot, part], xo_recv.at[there, part], x_peer,
        )

    tables = [
        pltpu.make_async_copy(source.at[which], target, table_sem.at[index])
        for index, (source, which, target) in enumerate((
            (sent_hi_all, side, sent_hi), (sent_lo_all, side, sent_lo),
            (own_hi_all, side, own_hi), (own_lo_all, side, own_lo),
            (fill_hi_all, 1 - side, fill_hi), (fill_lo_all, 1 - side, fill_lo),
        ))
    ]
    in_rows = inb.reshape(2 * 2 * points * SUBLANES, LANES)
    out_rows = out.reshape(2 * modes * groups * 2 * SUBLANES, LANES)
    k_rows = groups * 2 * SUBLANES

    def arrange(t):
        group, piece = t // PIECES, lax.rem(t, PIECES)

        @pl.when(piece == 0)
        def _():
            for half in range(2):
                load(group, half).wait()

        @pl.when(t >= OTHER_SLOTS)
        def _():
            for part in range(2):
                samples_x(t - OTHER_SLOTS, place, part).wait_send()

        slot, spare = lax.rem(t, GRID_SLOTS), lax.rem(t, OTHER_SLOTS)

        def tile(index, carry):
            first = pl.multiple_of(index * TILE, TILE)
            for field in range(FIELDS):
                lanes = pl.ds(field * LANES, LANES)

                def read(half):
                    base = ((lax.rem(group, 2) * 2 + half) * points + first) * SUBLANES
                    return in_rows[pl.ds(base + FIELDS * piece + field, TILE, stride=SUBLANES), :]

                other[spare, pl.ds(first, TILE), lanes] = read(1 - x)
                grid[slot, place, pl.ds(first, TILE), lanes] = read(x)
            return carry

        lax.fori_loop(0, points // TILE, tile, 0)

        @pl.when((piece == PIECES - 1) & (group + 2 < groups))
        def _():
            for half in range(2):
                load(group + 2, half).start()

    def store(t, half, ref):
        group, piece = t // PIECES, lax.rem(t, PIECES)
        share = modes // 2
        for parity in range(2):
            for part in range(2):
                for field in range(FIELDS):
                    first = (part * modes + parity) * k_rows
                    base = first + (group * 2 + half) * SUBLANES + FIELDS * piece + field
                    out_rows[pl.ds(base, share, stride=2 * k_rows), :] = ref[
                        pl.ds((parity * 2 + part) * share, share), pl.ds(field * LANES, LANES)
                    ]

    def dot3(a_hi, a_lo, b_hi, b_lo):
        dot = functools.partial(jnp.dot, preferred_element_type=jnp.float32)
        return dot(a_hi, b_hi) + dot(a_hi, b_lo) + dot(a_lo, b_hi)

    def encode(t):
        slot, here = lax.rem(t, GRID_SLOTS), lax.rem(t, CODED_SLOTS)
        for which in range(SIDE):

            def tile(index, carry):
                first = pl.multiple_of(index * 32, 32)
                high, low = split(grid[slot, which, pl.ds(first, 32), :])
                rows = pl.ds(pl.multiple_of(which * points + first, 32), 32)
                x_hi[rows, :] = high
                x_lo[rows, :] = low
                return carry

            lax.fori_loop(0, points // 32, tile, 0)

        @pl.when(t >= CODED_SLOTS)
        def _():
            for part in range(2):
                code(t - CODED_SLOTS, part, row).wait_send()

        coded[here] = dot3(sent_hi[...], sent_lo[...], x_hi[...], x_lo[...])
        for part in range(2):
            code(t, part, row).start()

    def own_modes(t):
        slot = lax.rem(t, DONE_SLOTS)

        @pl.when(t >= DONE_SLOTS)
        def _():
            for part in range(2):
                for which in range(2):
                    modes_z(t - DONE_SLOTS, which, 1 - row, part).wait_send()
                modes_x(t - DONE_SLOTS, part).wait_send()

        def block(which, carry):
            rows = pl.ds(pl.multiple_of(which * points, points), points)
            done[slot, which] = dot3(own_hi[rows, :], own_lo[rows, :], x_hi[...], x_lo[...])
            return carry

        lax.fori_loop(0, SIDE, block, 0)

    def add_evens(t, line):
        slot, there = lax.rem(t, DONE_SLOTS), lax.rem(t, ARRIVED_SLOTS)
        for which in range(2):
            first = pl.multiple_of(evens(line) + which * modes, SUBLANES)
            done[slot, line * 2 + which, :modes] += arrived[there, pl.ds(first, modes), :]

    def decode(t):
        slot, there = lax.rem(t, DONE_SLOTS), lax.rem(t, ARRIVED_SLOTS)

        def tile(index, carry):
            rows = pl.ds(pl.multiple_of(index * 32, 32), 32)
            high, low = split(arrived[there, rows, :])
            c_hi[rows, :] = high
            c_lo[rows, :] = low
            return carry

        lax.fori_loop(0, padded // 32, tile, 0)
        odd = dot3(fill_hi[...], fill_lo[...], c_hi[...], c_lo[...])
        for which in range(SIDE):
            done[slot, which, modes:] += odd[which * modes : (which + 1) * modes]

    for half in range(2):
        load(0, half).start()

    arrived[:, rank:padded] = jnp.zeros((arrived.shape[0], padded - rank, arrived.shape[2]), jnp.float32)
    barrier = pltpu.get_barrier_semaphore()
    for peer in (x_peer, z_peer):
        pl.semaphore_signal(
            barrier, inc=1, device_id={"lon": peer}, device_id_type=pl.DeviceIdType.MESH
        )

    @pl.when(inner)
    def _():
        pl.semaphore_signal(
            barrier, inc=1, device_id={"lon": m_peer}, device_id_type=pl.DeviceIdType.MESH
        )

    arrange(0)

    @pl.when(inner)
    def _():
        pl.semaphore_wait(barrier, 3)

    @pl.when(outer)
    def _():
        pl.semaphore_wait(barrier, 2)

    @pl.when(outer)
    def _():
        for part in range(2):
            samples_z(0, x, row, part).start()

    for part in range(2):
        samples_x(0, place, part).start()

    @pl.when(inner)
    def _():
        for copy in tables:
            copy.start()

    for half in range(2):
        load(1, half).start()

    for t in range(1, AHEAD):
        arrange(t)
        for part in range(2):
            samples_x(t, place, part).start()

    def step(i, carry):
        @pl.when(outer & (i >= SENT_LAG) & (i < chunks + SENT_LAG))
        def _():
            for which in range(2):
                for part in range(2):
                    samples_z(i - SENT_LAG, which, row, part).wait_send()

        @pl.when(i + AHEAD < chunks)
        def _():
            arrange(i + AHEAD)
            for part in range(2):
                samples_x(i + AHEAD, place, part).start()

        @pl.when(outer & (i < chunks))
        def _():
            for part in range(2):
                samples_x(i, beside, part).wait_recv()
                samples_z(i, 1 - x, row, part).start()

            @pl.when(i + 1 < chunks)
            def _():
                for part in range(2):
                    samples_z(i + 1, x, row, part).start()

        @pl.when(outer & (i >= LAG) & (i < chunks + LAG))
        def _():
            t = i - LAG
            for part in range(2):
                modes_z(t, 1 - x, row, part).wait_recv()
                modes_x(t, part).start()
            for part in range(2):
                modes_z(t, x, row, part).wait_recv()
            store(t, x, done.at[lax.rem(t, DONE_SLOTS), place])

        @pl.when(outer & (i >= LAG + 1) & (i < chunks + LAG + 1))
        def _():
            t = i - LAG - 1
            for part in range(2):
                modes_x(t, part).wait_send()
                modes_x(t, part).wait_recv()
            store(t, 1 - x, cross.at[lax.rem(t, CROSS_SLOTS)])

        @pl.when(inner & (i < chunks))
        def _():
            for part in range(2):
                samples_x(i, beside, part).wait_recv()
                for which in range(2):
                    samples_z(i, which, 1 - row, part).wait_recv()

            @pl.when(i == 0)
            def _():
                for copy in tables:
                    copy.wait()

            encode(i)
            own_modes(i)

        @pl.when(inner & (i >= 1) & (i < chunks + 1))
        def _():
            t = i - 1
            code(t, 0, 1 - row).wait_recv()
            add_evens(t, 1 - row)
            for which in (1 - x, x):
                modes_z(t, which, 1 - row, 0).start()
            code(t, 1, 1 - row).wait_recv()
            add_evens(t, row)
            modes_x(t, 0).start()
            decode(t)
            modes_z(t, 1 - x, 1 - row, 1).start()
            modes_x(t, 1).start()
            modes_z(t, x, 1 - row, 1).start()
            store(t, x, done.at[lax.rem(t, DONE_SLOTS), place])

        @pl.when(inner & (i >= 2) & (i < chunks + 2))
        def _():
            t = i - 2
            for part in range(2):
                modes_x(t, part).wait_recv()
            store(t, 1 - x, cross.at[lax.rem(t, CROSS_SLOTS)])

        return carry

    lax.fori_loop(0, chunks + LAG + 1, step, 0)

    for part in range(2):
        for back in range(OTHER_SLOTS):
            samples_x(chunks - 1 - back, place, part).wait_send()

    @pl.when(inner)
    def _():
        for part in range(2):
            for back in range(CODED_SLOTS):
                code(chunks - 1 - back, part, row).wait_send()
            for back in range(DONE_SLOTS):
                for which in range(2):
                    modes_z(chunks - 1 - back, which, 1 - row, part).wait_send()
                modes_x(chunks - 1 - back, part).wait_send()


def fused_local(state):
    points, fields, lat_dev = state.shape
    modes = points // 2
    groups = fields // SUBLANES
    chunks = groups * PIECES
    tables = all_tables(points)
    padded = tables[2].shape[1]
    rank = RADIX * points // 4 + EXTRA
    vmem = pl.BlockSpec(memory_space=pltpu.VMEM)
    hbm = pl.BlockSpec(memory_space=pl.ANY)
    wide = FIELDS * LANES
    dma = pltpu.SemaphoreType.DMA

    def f32(*shape):
        return pltpu.VMEM(shape, jnp.float32)

    def bf16(*shape):
        return pltpu.VMEM(shape, jnp.bfloat16)

    result = pl.pallas_call(
        functools.partial(kernel, chunks, rank),
        out_shape=pltpu.VMEM((2, modes, groups, 2, SUBLANES, LANES), jnp.float32),
        in_specs=[hbm] * (1 + len(tables)),
        out_specs=vmem,
        scratch_shapes=[
            f32(2, 2, points, SUBLANES, LANES),
            f32(GRID_SLOTS, SIDE, points, wide),
            f32(OTHER_SLOTS, points, wide),
            f32(CODED_SLOTS, padded, wide),
            f32(ARRIVED_SLOTS, padded, wide),
            f32(DONE_SLOTS, SIDE, points, wide),
            f32(CROSS_SLOTS, points, wide),
            *[bf16(*table.shape[1:]) for table in tables],
            bf16(SIDE * points, wide),
            bf16(SIDE * points, wide),
            bf16(padded, wide),
            bf16(padded, wide),
            dma((2, 2)),
            dma((len(tables),)),
            dma((OTHER_SLOTS, 2)),
            dma((GRID_SLOTS, 2)),
            dma((GRID_SLOTS, 2, 2)),
            dma((GRID_SLOTS, 2, 2)),
            dma((CODED_SLOTS, 2)),
            dma((ARRIVED_SLOTS, 2)),
            dma((DONE_SLOTS, 2, 2)),
            dma((DONE_SLOTS, 2, 2)),
            dma((DONE_SLOTS, 2)),
            dma((CROSS_SLOTS, 2)),
        ],
        compiler_params=pltpu.CompilerParams(
            collective_id=0, has_side_effects=True, vmem_limit_bytes=VMEM_LIMIT
        ),
    )(state, *tables)
    return result.transpose(0, 1, 2, 4, 3, 5).reshape(2, modes, fields, lat_dev)


def solution(mesh):
    devices = mesh.shape["lon"]

    def local(state):
        points, fields, lat_dev = state.shape
        fits = (
            devices == RADIX
            and fields == RADIX * SUBLANES
            and points == 2 * LANES
            and lat_dev == 2 * LANES
        )
        return fused_local(state) if fits else dense_local(state)

    return jax.shard_map(
        local,
        mesh=mesh,
        in_specs=(P("lon", None, "lat"),),
        out_specs=P(None, "lon", None, "lat"),
        check_vma=False,
    )
```

```python
import functools
import math

import jax
import jax.numpy as jnp
import numpy as np
from jax import lax
from jax.experimental import pallas as pl
from jax.experimental.pallas import tpu as pltpu
from jax.sharding import PartitionSpec as P

RADIX = 8
LANES = 128
SUBLANES = 8
TILE = 16
SIDE = RADIX // 2
FIELDS = 1
PIECES = SUBLANES // FIELDS
AHEAD = 2
SENT_LAG = 2
EXTRA = 24
LAG = 7
GRID_SLOTS = 9
OTHER_SLOTS = 4
CODED_SLOTS = 3
ARRIVED_SLOTS = 4
DONE_SLOTS = 9
CROSS_SLOTS = 5
VMEM_LIMIT = 46 * 1024 * 1024


def phase_angle(first_index, second_index, period):
    product = first_index * second_index % period
    return product.astype(jnp.float32) * (2.0 * math.pi / period)


def dense_spectrum(gathered, factor):
    lon_count = gathered.shape[0]
    mode_count = lon_count // 2
    wavenum = lax.broadcasted_iota(jnp.int32, (mode_count, lon_count), 0)
    longitude = lax.broadcasted_iota(jnp.int32, (mode_count, lon_count), 1)
    angles = phase_angle(wavenum, longitude, lon_count)
    real_part = jnp.dot(
        jnp.cos(angles) * factor,
        gathered,
        precision=lax.Precision.HIGHEST,
        preferred_element_type=jnp.float32,
    )
    imag_part = jnp.dot(
        -jnp.sin(angles) * factor,
        gathered,
        precision=lax.Precision.HIGHEST,
        preferred_element_type=jnp.float32,
    )
    return jnp.stack([real_part, imag_part])


def dense_local(state):
    lon_dev, fields, lat_dev = state.shape
    devices = lax.axis_size("lon")
    columns = state.reshape(lon_dev, fields * lat_dev)
    factor = 1.0 / math.sqrt(lon_dev * devices)
    gathered = lax.all_to_all(columns, "lon", split_axis=1, concat_axis=0, tiled=True)
    spectrum = dense_spectrum(gathered, factor)
    shares = lax.all_to_all(spectrum, "lon", split_axis=1, concat_axis=2, tiled=True)
    return shares.reshape(2, shares.shape[1], fields, lat_dev)


def split(value):
    high = value.astype(jnp.bfloat16)
    return high, (value - high.astype(jnp.float32)).astype(jnp.bfloat16)


def split_table(table):
    high = table.astype(jnp.bfloat16)
    return high, (table - high.astype(np.float64)).astype(jnp.bfloat16)


def dft_rows(wavenums, places, count):
    angle = 2.0 * np.pi / count * (wavenums[:, None] * places[None] % count)
    scale = 1.0 / math.sqrt(count)
    return scale * np.cos(angle), -scale * np.sin(angle)


def by_owner(parts):
    shaped = [part.reshape(SIDE, -1, part.shape[1]) for part in parts]
    return np.stack(shaped, 1).reshape(-1, parts[0].shape[1])


def side_tables(points, side):
    count, band = RADIX * points, RADIX * points // 4
    places = side * (count // 2) + np.arange(count // 2)
    step = 2 * np.arange(band // 2)

    def rows(first):
        return by_owner(dft_rows(first + step, places, count))

    own = [rows(side * band + parity).reshape(SIDE, 1, -1, count // 2) for parity in range(2)]
    own = np.concatenate(own, 1).reshape(2 * band, count // 2)
    even, odd = rows((1 - side) * band), rows((1 - side) * band + 1)
    power = (even * even).sum(1)
    spread = (odd @ even.T) * np.where(power > 1e-9, 1.0 / np.maximum(power, 1e-9), 0.0)
    left = odd - spread @ even
    rest, basis = left, []
    for _ in range(EXTRA):
        row, column = np.unravel_index(np.argmax(np.abs(rest)), rest.shape)
        basis.append(rest[row] / np.abs(rest[row]).max())
        rest = rest - np.outer(rest[:, column] / rest[row, column], rest[row])
    extra = np.linalg.qr(np.stack(basis, 1))[0].T
    mix = left @ extra.T
    rank, padded = band + EXTRA, -(-(band + EXTRA) // 16) * 16
    sent = np.zeros((padded, count // 2))
    sent[:rank] = np.concatenate([even[: band // 2], extra, even[band // 2 :]])
    fill = np.zeros((band, padded))
    fill[:, :rank] = np.concatenate([spread[:, : band // 2], mix, spread[:, band // 2 :]], 1)
    return own, sent, fill


def all_tables(points):
    sides = [side_tables(points, side) for side in range(2)]
    out = []
    for tables in zip(*sides):
        for piece in split_table(np.stack(tables)):
            out.append(jnp.asarray(piece))
    return out


def kernel(
    chunks, rank,
    state, own_hi_all, own_lo_all, sent_hi_all, sent_lo_all, fill_hi_all, fill_lo_all, out,
    inb, grid, other, coded, arrived, done, cross,
    own_hi, own_lo, sent_hi, sent_lo, fill_hi, fill_lo, x_hi, x_lo, c_hi, c_lo,
    in_sem, table_sem, xs_send, xs_recv, zs_send, zs_recv, m_send, m_recv,
    zo_send, zo_recv, xo_send, xo_recv,
):
    points = state.shape[0]
    modes = points // 2
    groups = chunks // PIECES
    padded, band = coded.shape[1], rank - EXTRA
    me = lax.axis_index("lon")
    z, x = me // 2, lax.rem(me, 2)
    row, side = lax.rem(z, 2), z // 2
    place = lax.rem(me, SIDE)
    beside = place + 1 - 2 * x
    inner = lax.rem((z + 1) // 2, 2) == 1
    outer = lax.rem((z + 1) // 2, 2) == 0
    x_peer = me + 1 - 2 * x
    z_peer = me + 2 - 4 * row
    m_peer = (3 - z) * 2 + x

    def remote(source, target, send, recv, peer):
        return pltpu.make_async_remote_copy(
            src_ref=source, dst_ref=target, send_sem=send, recv_sem=recv,
            device_id={"lon": peer}, device_id_type=pl.DeviceIdType.MESH,
        )

    def load(group, half):
        slot = lax.rem(group, 2)
        fields = pl.ds(pl.multiple_of(group * SUBLANES, SUBLANES), SUBLANES)
        return pltpu.make_async_copy(
            state.at[:, fields, half * LANES : (half + 1) * LANES],
            inb.at[slot, half], in_sem.at[slot, half],
        )

    def cut(part):
        return pl.ds(part * modes, modes)

    def samples_x(t, target_place, part):
        here, slot = lax.rem(t, OTHER_SLOTS), lax.rem(t, GRID_SLOTS)
        return remote(
            other.at[here, cut(part)], grid.at[slot, target_place, cut(part)],
            xs_send.at[here, part], xs_recv.at[slot, part], x_peer,
        )

    def samples_z(t, which, line, part):
        slot = lax.rem(t, GRID_SLOTS)
        ref = grid.at[slot, line * 2 + which, cut(part)]
        return remote(ref, ref, zs_send.at[slot, which, part], zs_recv.at[slot, which, part], z_peer)

    def evens(line):
        return line * (band // 2 + EXTRA)

    def code(t, part, line):
        if part == 0:
            rows = pl.ds(evens(line), band // 2)
        else:
            rows = pl.ds((1 - line) * (band // 2), band // 2 + EXTRA)
        here, there = lax.rem(t, CODED_SLOTS), lax.rem(t, ARRIVED_SLOTS)
        return remote(
            coded.at[here, rows], arrived.at[there, rows],
            m_send.at[here, part], m_recv.at[there, part], m_peer,
        )

    def modes_z(t, which, line, part):
        slot = lax.rem(t, DONE_SLOTS)
        ref = done.at[slot, line * 2 + which, cut(part)]
        return remote(ref, ref, zo_send.at[slot, which, part], zo_recv.at[slot, which, part], z_peer)

    def modes_x(t, part):
        slot, there = lax.rem(t, DONE_SLOTS), lax.rem(t, CROSS_SLOTS)
        return remote(
            done.at[slot, beside, cut(part)], cross.at[there, cut(part)],
            xo_send.at[slot, part], xo_recv.at[there, part], x_peer,
        )

    tables = [
        pltpu.make_async_copy(source.at[which], target, table_sem.at[index])
        for index, (source, which, target) in enumerate((
            (sent_hi_all, side, sent_hi), (sent_lo_all, side, sent_lo),
            (own_hi_all, side, own_hi), (own_lo_all, side, own_lo),
            (fill_hi_all, 1 - side, fill_hi), (fill_lo_all, 1 - side, fill_lo),
        ))
    ]
    in_rows = inb.reshape(2 * 2 * points * SUBLANES, LANES)
    out_rows = out.reshape(2 * modes * groups * 2 * SUBLANES, LANES)
    k_rows = groups * 2 * SUBLANES

    def arrange(t):
        group, piece = t // PIECES, lax.rem(t, PIECES)

        @pl.when(piece == 0)
        def _():
            for half in range(2):
                load(group, half).wait()

        @pl.when(t >= OTHER_SLOTS)
        def _():
            for part in range(2):
                samples_x(t - OTHER_SLOTS, place, part).wait_send()

        slot, spare = lax.rem(t, GRID_SLOTS), lax.rem(t, OTHER_SLOTS)

        def tile(index, carry):
            first = pl.multiple_of(index * TILE, TILE)
            for field in range(FIELDS):
                lanes = pl.ds(field * LANES, LANES)

                def read(half):
                    base = ((lax.rem(group, 2) * 2 + half) * points + first) * SUBLANES
                    return in_rows[pl.ds(base + FIELDS * piece + field, TILE, stride=SUBLANES), :]

                other[spare, pl.ds(first, TILE), lanes] = read(1 - x)
                grid[slot, place, pl.ds(first, TILE), lanes] = read(x)
            return carry

        lax.fori_loop(0, points // TILE, tile, 0)

        @pl.when((piece == PIECES - 1) & (group + 2 < groups))
        def _():
            for half in range(2):
                load(group + 2, half).start()

    def store(t, half, ref):
        group, piece = t // PIECES, lax.rem(t, PIECES)
        share = modes // 2
        for parity in range(2):
            for part in range(2):
                for field in range(FIELDS):
                    first = (part * modes + parity) * k_rows
                    base = first + (group * 2 + half) * SUBLANES + FIELDS * piece + field
                    out_rows[pl.ds(base, share, stride=2 * k_rows), :] = ref[
                        pl.ds((parity * 2 + part) * share, share), pl.ds(field * LANES, LANES)
                    ]

    def dot3(a_hi, a_lo, b_hi, b_lo):
        dot = functools.partial(jnp.dot, preferred_element_type=jnp.float32)
        return dot(a_hi, b_hi) + dot(a_hi, b_lo) + dot(a_lo, b_hi)

    def encode(t):
        slot, here = lax.rem(t, GRID_SLOTS), lax.rem(t, CODED_SLOTS)
        for which in range(SIDE):

            def tile(index, carry):
                first = pl.multiple_of(index * 32, 32)
                high, low = split(grid[slot, which, pl.ds(first, 32), :])
                rows = pl.ds(pl.multiple_of(which * points + first, 32), 32)
                x_hi[rows, :] = high
                x_lo[rows, :] = low
                return carry

            lax.fori_loop(0, points // 32, tile, 0)

        @pl.when(t >= CODED_SLOTS)
        def _():
            for part in range(2):
                code(t - CODED_SLOTS, part, row).wait_send()

        coded[here] = dot3(sent_hi[...], sent_lo[...], x_hi[...], x_lo[...])
        for part in range(2):
            code(t, part, row).start()

    def own_modes(t):
        slot = lax.rem(t, DONE_SLOTS)

        @pl.when(t >= DONE_SLOTS)
        def _():
            for part in range(2):
                for which in range(2):
                    modes_z(t - DONE_SLOTS, which, 1 - row, part).wait_send()
                modes_x(t - DONE_SLOTS, part).wait_send()

        def block(which, carry):
            rows = pl.ds(pl.multiple_of(which * points, points), points)
            done[slot, which] = dot3(own_hi[rows, :], own_lo[rows, :], x_hi[...], x_lo[...])
            return carry

        lax.fori_loop(0, SIDE, block, 0)

    def add_evens(t, line):
        slot, there = lax.rem(t, DONE_SLOTS), lax.rem(t, ARRIVED_SLOTS)
        for which in range(2):
            first = pl.multiple_of(evens(line) + which * modes, SUBLANES)
            done[slot, line * 2 + which, :modes] += arrived[there, pl.ds(first, modes), :]

    def decode(t):
        slot, there = lax.rem(t, DONE_SLOTS), lax.rem(t, ARRIVED_SLOTS)

        def tile(index, carry):
            rows = pl.ds(pl.multiple_of(index * 32, 32), 32)
            high, low = split(arrived[there, rows, :])
            c_hi[rows, :] = high
            c_lo[rows, :] = low
            return carry

        lax.fori_loop(0, padded // 32, tile, 0)
        odd = dot3(fill_hi[...], fill_lo[...], c_hi[...], c_lo[...])
        for which in range(SIDE):
            done[slot, which, modes:] += odd[which * modes : (which + 1) * modes]

    for half in range(2):
        load(0, half).start()

    arrived[:, rank:padded] = jnp.zeros((arrived.shape[0], padded - rank, arrived.shape[2]), jnp.float32)
    barrier = pltpu.get_barrier_semaphore()
    for peer in (x_peer, z_peer):
        pl.semaphore_signal(
            barrier, inc=1, device_id={"lon": peer}, device_id_type=pl.DeviceIdType.MESH
        )

    @pl.when(inner)
    def _():
        pl.semaphore_signal(
            barrier, inc=1, device_id={"lon": m_peer}, device_id_type=pl.DeviceIdType.MESH
        )

    arrange(0)

    @pl.when(inner)
    def _():
        pl.semaphore_wait(barrier, 3)

    @pl.when(outer)
    def _():
        pl.semaphore_wait(barrier, 2)

    @pl.when(outer)
    def _():
        for part in range(2):
            samples_z(0, x, row, part).start()

    for part in range(2):
        samples_x(0, place, part).start()

    @pl.when(inner)
    def _():
        for copy in tables:
            copy.start()

    for half in range(2):
        load(1, half).start()

    for t in range(1, AHEAD):
        arrange(t)
        for part in range(2):
            samples_x(t, place, part).start()

    def step(i, carry):
        @pl.when(outer & (i >= SENT_LAG) & (i < chunks + SENT_LAG))
        def _():
            for which in range(2):
                for part in range(2):
                    samples_z(i - SENT_LAG, which, row, part).wait_send()

        @pl.when(i + AHEAD < chunks)
        def _():
            arrange(i + AHEAD)
            for part in range(2):
                samples_x(i + AHEAD, place, part).start()

        @pl.when(outer & (i < chunks))
        def _():
            for part in range(2):
                samples_x(i, beside, part).wait_recv()
                samples_z(i, 1 - x, row, part).start()

            @pl.when(i + 1 < chunks)
            def _():
                for part in range(2):
                    samples_z(i + 1, x, row, part).start()

        @pl.when(outer & (i >= LAG) & (i < chunks + LAG))
        def _():
            t = i - LAG
            for part in range(2):
                modes_z(t, 1 - x, row, part).wait_recv()
                modes_x(t, part).start()
            for part in range(2):
                modes_z(t, x, row, part).wait_recv()
            store(t, x, done.at[lax.rem(t, DONE_SLOTS), place])

        @pl.when(outer & (i >= LAG + 1) & (i < chunks + LAG + 1))
        def _():
            t = i - LAG - 1
            for part in range(2):
                modes_x(t, part).wait_send()
                modes_x(t, part).wait_recv()
            store(t, 1 - x, cross.at[lax.rem(t, CROSS_SLOTS)])

        @pl.when(inner & (i < chunks))
        def _():
            for part in range(2):
                samples_x(i, beside, part).wait_recv()
                for which in range(2):
                    samples_z(i, which, 1 - row, part).wait_recv()

            @pl.when(i == 0)
            def _():
                for copy in tables:
                    copy.wait()

            encode(i)
            own_modes(i)

        @pl.when(inner & (i >= 1) & (i < chunks + 1))
        def _():
            t = i - 1
            code(t, 0, 1 - row).wait_recv()
            add_evens(t, 1 - row)
            for which in (1 - x, x):
                modes_z(t, which, 1 - row, 0).start()
            code(t, 1, 1 - row).wait_recv()
            add_evens(t, row)
            modes_x(t, 0).start()
            decode(t)
            modes_z(t, 1 - x, 1 - row, 1).start()
            modes_x(t, 1).start()
            modes_z(t, x, 1 - row, 1).start()
            store(t, x, done.at[lax.rem(t, DONE_SLOTS), place])

        @pl.when(inner & (i >= 2) & (i < chunks + 2))
        def _():
            t = i - 2
            for part in range(2):
                modes_x(t, part).wait_recv()
            store(t, 1 - x, cross.at[lax.rem(t, CROSS_SLOTS)])

        return carry

    lax.fori_loop(0, chunks + LAG + 1, step, 0)

    for part in range(2):
        for back in range(OTHER_SLOTS):
            samples_x(chunks - 1 - back, place, part).wait_send()

    @pl.when(inner)
    def _():
        for part in range(2):
            for back in range(CODED_SLOTS):
                code(chunks - 1 - back, part, row).wait_send()
            for back in range(DONE_SLOTS):
                for which in range(2):
                    modes_z(chunks - 1 - back, which, 1 - row, part).wait_send()
                modes_x(chunks - 1 - back, part).wait_send()


def fused_local(state):
    points, fields, lat_dev = state.shape
    modes = points // 2
    groups = fields // SUBLANES
    chunks = groups * PIECES
    tables = all_tables(points)
    padded = tables[2].shape[1]
    rank = RADIX * points // 4 + EXTRA
    vmem = pl.BlockSpec(memory_space=pltpu.VMEM)
    hbm = pl.BlockSpec(memory_space=pl.ANY)
    wide = FIELDS * LANES
    dma = pltpu.SemaphoreType.DMA

    def f32(*shape):
        return pltpu.VMEM(shape, jnp.float32)

    def bf16(*shape):
        return pltpu.VMEM(shape, jnp.bfloat16)

    result = pl.pallas_call(
        functools.partial(kernel, chunks, rank),
        out_shape=pltpu.VMEM((2, modes, groups, 2, SUBLANES, LANES), jnp.float32),
        in_specs=[hbm] * (1 + len(tables)),
        out_specs=vmem,
        scratch_shapes=[
            f32(2, 2, points, SUBLANES, LANES),
            f32(GRID_SLOTS, SIDE, points, wide),
            f32(OTHER_SLOTS, points, wide),
            f32(CODED_SLOTS, padded, wide),
            f32(ARRIVED_SLOTS, padded, wide),
            f32(DONE_SLOTS, SIDE, points, wide),
            f32(CROSS_SLOTS, points, wide),
            *[bf16(*table.shape[1:]) for table in tables],
            bf16(SIDE * points, wide),
            bf16(SIDE * points, wide),
            bf16(padded, wide),
            bf16(padded, wide),
            dma((2, 2)),
            dma((len(tables),)),
            dma((OTHER_SLOTS, 2)),
            dma((GRID_SLOTS, 2)),
            dma((GRID_SLOTS, 2, 2)),
            dma((GRID_SLOTS, 2, 2)),
            dma((CODED_SLOTS, 2)),
            dma((ARRIVED_SLOTS, 2)),
            dma((DONE_SLOTS, 2, 2)),
            dma((DONE_SLOTS, 2, 2)),
            dma((DONE_SLOTS, 2)),
            dma((CROSS_SLOTS, 2)),
        ],
        compiler_params=pltpu.CompilerParams(
            collective_id=0, has_side_effects=True, vmem_limit_bytes=VMEM_LIMIT
        ),
    )(state, *tables)
    return result.transpose(0, 1, 2, 4, 3, 5).reshape(2, modes, fields, lat_dev)


def solution(mesh):
    devices = mesh.shape["lon"]

    def local(state):
        points, fields, lat_dev = state.shape
        fits = (
            devices == RADIX
            and fields == RADIX * SUBLANES
            and points == 2 * LANES
            and lat_dev == 2 * LANES
        )
        return fused_local(state) if fits else dense_local(state)

    return jax.shard_map(
        local,
        mesh=mesh,
        in_specs=(P("lon", None, "lat"),),
        out_specs=P(None, "lon", None, "lat"),
        check_vma=False,
    )
```

```python
import functools
import math

import jax
import jax.numpy as jnp
import numpy as np
from jax import lax
from jax.experimental import pallas as pl
from jax.experimental.pallas import tpu as pltpu
from jax.sharding import PartitionSpec as P

RADIX = 8
LANES = 128
SUBLANES = 8
TILE = 16
SIDE = RADIX // 2
FIELDS = 1
PIECES = SUBLANES // FIELDS
AHEAD = 2
SLABS = 4
SENT_LAG = 2
EXTRA = 24
LAG = 7
GRID_SLOTS = 9
OTHER_SLOTS = 4
CODED_SLOTS = 3
ARRIVED_SLOTS = 4
DONE_SLOTS = 9
CROSS_SLOTS = 5
VMEM_LIMIT = 46 * 1024 * 1024


def phase_angle(first_index, second_index, period):
    product = first_index * second_index % period
    return product.astype(jnp.float32) * (2.0 * math.pi / period)


def dense_spectrum(gathered, factor):
    lon_count = gathered.shape[0]
    mode_count = lon_count // 2
    wavenum = lax.broadcasted_iota(jnp.int32, (mode_count, lon_count), 0)
    longitude = lax.broadcasted_iota(jnp.int32, (mode_count, lon_count), 1)
    angles = phase_angle(wavenum, longitude, lon_count)
    real_part = jnp.dot(
        jnp.cos(angles) * factor,
        gathered,
        precision=lax.Precision.HIGHEST,
        preferred_element_type=jnp.float32,
    )
    imag_part = jnp.dot(
        -jnp.sin(angles) * factor,
        gathered,
        precision=lax.Precision.HIGHEST,
        preferred_element_type=jnp.float32,
    )
    return jnp.stack([real_part, imag_part])


def dense_local(state):
    lon_dev, fields, lat_dev = state.shape
    devices = lax.axis_size("lon")
    columns = state.reshape(lon_dev, fields * lat_dev)
    factor = 1.0 / math.sqrt(lon_dev * devices)
    gathered = lax.all_to_all(columns, "lon", split_axis=1, concat_axis=0, tiled=True)
    spectrum = dense_spectrum(gathered, factor)
    shares = lax.all_to_all(spectrum, "lon", split_axis=1, concat_axis=2, tiled=True)
    return shares.reshape(2, shares.shape[1], fields, lat_dev)


def split(value):
    high = value.astype(jnp.bfloat16)
    return high, (value - high.astype(jnp.float32)).astype(jnp.bfloat16)


def split_table(table):
    high = table.astype(jnp.bfloat16)
    return high, (table - high.astype(np.float64)).astype(jnp.bfloat16)


def dft_rows(wavenums, places, count):
    angle = 2.0 * np.pi / count * (wavenums[:, None] * places[None] % count)
    scale = 1.0 / math.sqrt(count)
    return scale * np.cos(angle), -scale * np.sin(angle)


def by_owner(parts):
    shaped = [part.reshape(SIDE, -1, part.shape[1]) for part in parts]
    return np.stack(shaped, 1).reshape(-1, parts[0].shape[1])


def side_tables(points, side):
    count, band = RADIX * points, RADIX * points // 4
    places = side * (count // 2) + np.arange(count // 2)
    step = 2 * np.arange(band // 2)

    def rows(first):
        return by_owner(dft_rows(first + step, places, count))

    own = [rows(side * band + parity).reshape(SIDE, 1, -1, count // 2) for parity in range(2)]
    own = np.concatenate(own, 1).reshape(2 * band, count // 2)
    even, odd = rows((1 - side) * band), rows((1 - side) * band + 1)
    power = (even * even).sum(1)
    spread = (odd @ even.T) * np.where(power > 1e-9, 1.0 / np.maximum(power, 1e-9), 0.0)
    left = odd - spread @ even
    rest, basis = left, []
    for _ in range(EXTRA):
        row, column = np.unravel_index(np.argmax(np.abs(rest)), rest.shape)
        basis.append(rest[row] / np.abs(rest[row]).max())
        rest = rest - np.outer(rest[:, column] / rest[row, column], rest[row])
    extra = np.linalg.qr(np.stack(basis, 1))[0].T
    mix = left @ extra.T
    rank, padded = band + EXTRA, -(-(band + EXTRA) // 16) * 16
    sent = np.zeros((padded, count // 2))
    sent[:rank] = np.concatenate([even[: band // 2], extra, even[band // 2 :]])
    fill = np.zeros((band, padded))
    fill[:, :rank] = np.concatenate([spread[:, : band // 2], mix, spread[:, band // 2 :]], 1)
    return own, sent, fill


def all_tables(points):
    sides = [side_tables(points, side) for side in range(2)]
    out = []
    for tables in zip(*sides):
        for piece in split_table(np.stack(tables)):
            out.append(jnp.asarray(piece))
    return out


def kernel(
    chunks, rank,
    state, own_hi_all, own_lo_all, sent_hi_all, sent_lo_all, fill_hi_all, fill_lo_all, out,
    inb, grid, other, coded, arrived, done, cross,
    own_hi, own_lo, sent_hi, sent_lo, fill_hi, fill_lo, x_hi, x_lo, c_hi, c_lo,
    in_sem, table_sem, xs_send, xs_recv, zs_send, zs_recv, m_send, m_recv,
    zo_send, zo_recv, xo_send, xo_recv,
):
    points = state.shape[0]
    modes = points // 2
    groups = chunks // PIECES
    padded, band = coded.shape[1], rank - EXTRA
    me = lax.axis_index("lon")
    z, x = me // 2, lax.rem(me, 2)
    row, side = lax.rem(z, 2), z // 2
    place = lax.rem(me, SIDE)
    beside = place + 1 - 2 * x
    inner = lax.rem((z + 1) // 2, 2) == 1
    outer = lax.rem((z + 1) // 2, 2) == 0
    x_peer = me + 1 - 2 * x
    z_peer = me + 2 - 4 * row
    m_peer = (3 - z) * 2 + x

    def remote(source, target, send, recv, peer):
        return pltpu.make_async_remote_copy(
            src_ref=source, dst_ref=target, send_sem=send, recv_sem=recv,
            device_id={"lon": peer}, device_id_type=pl.DeviceIdType.MESH,
        )

    def load(group, half):
        slot = lax.rem(group, 2)
        fields = pl.ds(pl.multiple_of(group * SUBLANES, SUBLANES), SUBLANES)
        return pltpu.make_async_copy(
            state.at[:, fields, half * LANES : (half + 1) * LANES],
            inb.at[slot, half], in_sem.at[slot, half],
        )

    def cut(part):
        return pl.ds(part * modes, modes)

    def slab(part):
        return pl.ds(part * (points // SLABS), points // SLABS)

    def samples_x(t, target_place, part):
        here, slot = lax.rem(t, OTHER_SLOTS), lax.rem(t, GRID_SLOTS)
        return remote(
            other.at[here, slab(part)], grid.at[slot, target_place, slab(part)],
            xs_send.at[here, part], xs_recv.at[slot, part], x_peer,
        )

    def samples_z(t, which, line, part):
        slot = lax.rem(t, GRID_SLOTS)
        ref = grid.at[slot, line * 2 + which, slab(part)]
        return remote(ref, ref, zs_send.at[slot, which, part], zs_recv.at[slot, which, part], z_peer)

    def evens(line):
        return line * (band // 2 + EXTRA)

    def code(t, part, line):
        if part == 0:
            rows = pl.ds(evens(line), band // 2)
        else:
            rows = pl.ds((1 - line) * (band // 2), band // 2 + EXTRA)
        here, there = lax.rem(t, CODED_SLOTS), lax.rem(t, ARRIVED_SLOTS)
        return remote(
            coded.at[here, rows], arrived.at[there, rows],
            m_send.at[here, part], m_recv.at[there, part], m_peer,
        )

    def modes_z(t, which, line, part):
        slot = lax.rem(t, DONE_SLOTS)
        ref = done.at[slot, line * 2 + which, cut(part)]
        return remote(ref, ref, zo_send.at[slot, which, part], zo_recv.at[slot, which, part], z_peer)

    def modes_x(t, part):
        slot, there = lax.rem(t, DONE_SLOTS), lax.rem(t, CROSS_SLOTS)
        return remote(
            done.at[slot, beside, cut(part)], cross.at[there, cut(part)],
            xo_send.at[slot, part], xo_recv.at[there, part], x_peer,
        )

    tables = [
        pltpu.make_async_copy(source.at[which], target, table_sem.at[index])
        for index, (source, which, target) in enumerate((
            (sent_hi_all, side, sent_hi), (sent_lo_all, side, sent_lo),
            (own_hi_all, side, own_hi), (own_lo_all, side, own_lo),
            (fill_hi_all, 1 - side, fill_hi), (fill_lo_all, 1 - side, fill_lo),
        ))
    ]
    in_rows = inb.reshape(2 * 2 * points * SUBLANES, LANES)
    out_rows = out.reshape(2 * modes * groups * 2 * SUBLANES, LANES)
    k_rows = groups * 2 * SUBLANES

    def arrange(t):
        group, piece = t // PIECES, lax.rem(t, PIECES)

        @pl.when(piece == 0)
        def _():
            for half in range(2):
                load(group, half).wait()

        @pl.when(t >= OTHER_SLOTS)
        def _():
            for part in range(SLABS):
                samples_x(t - OTHER_SLOTS, place, part).wait_send()

        slot, spare = lax.rem(t, GRID_SLOTS), lax.rem(t, OTHER_SLOTS)

        def tile(index, carry):
            first = pl.multiple_of(index * TILE, TILE)
            for field in range(FIELDS):
                lanes = pl.ds(field * LANES, LANES)

                def read(half):
                    base = ((lax.rem(group, 2) * 2 + half) * points + first) * SUBLANES
                    return in_rows[pl.ds(base + FIELDS * piece + field, TILE, stride=SUBLANES), :]

                other[spare, pl.ds(first, TILE), lanes] = read(1 - x)
                grid[slot, place, pl.ds(first, TILE), lanes] = read(x)
            return carry

        lax.fori_loop(0, points // TILE, tile, 0)

        @pl.when((piece == PIECES - 1) & (group + 2 < groups))
        def _():
            for half in range(2):
                load(group + 2, half).start()

    def store(t, half, ref):
        group, piece = t // PIECES, lax.rem(t, PIECES)
        share = modes // 2
        for parity in range(2):
            for part in range(2):
                for field in range(FIELDS):
                    first = (part * modes + parity) * k_rows
                    base = first + (group * 2 + half) * SUBLANES + FIELDS * piece + field
                    out_rows[pl.ds(base, share, stride=2 * k_rows), :] = ref[
                        pl.ds((parity * 2 + part) * share, share), pl.ds(field * LANES, LANES)
                    ]

    def dot3(a_hi, a_lo, b_hi, b_lo):
        dot = functools.partial(jnp.dot, preferred_element_type=jnp.float32)
        return dot(a_hi, b_hi) + dot(a_hi, b_lo) + dot(a_lo, b_hi)

    def encode(t):
        slot, here = lax.rem(t, GRID_SLOTS), lax.rem(t, CODED_SLOTS)
        for which in range(SIDE):

            def tile(index, carry):
                first = pl.multiple_of(index * 32, 32)
                high, low = split(grid[slot, which, pl.ds(first, 32), :])
                rows = pl.ds(pl.multiple_of(which * points + first, 32), 32)
                x_hi[rows, :] = high
                x_lo[rows, :] = low
                return carry

            lax.fori_loop(0, points // 32, tile, 0)

        @pl.when(t >= CODED_SLOTS)
        def _():
            for part in range(2):
                code(t - CODED_SLOTS, part, row).wait_send()

        coded[here] = dot3(sent_hi[...], sent_lo[...], x_hi[...], x_lo[...])
        for part in range(2):
            code(t, part, row).start()

    def own_modes(t):
        slot = lax.rem(t, DONE_SLOTS)

        @pl.when(t >= DONE_SLOTS)
        def _():
            for part in range(2):
                for which in range(2):
                    modes_z(t - DONE_SLOTS, which, 1 - row, part).wait_send()
                modes_x(t - DONE_SLOTS, part).wait_send()

        def block(which, carry):
            rows = pl.ds(pl.multiple_of(which * points, points), points)
            done[slot, which] = dot3(own_hi[rows, :], own_lo[rows, :], x_hi[...], x_lo[...])
            return carry

        lax.fori_loop(0, SIDE, block, 0)

    def add_evens(t, line):
        slot, there = lax.rem(t, DONE_SLOTS), lax.rem(t, ARRIVED_SLOTS)
        for which in range(2):
            first = pl.multiple_of(evens(line) + which * modes, SUBLANES)
            done[slot, line * 2 + which, :modes] += arrived[there, pl.ds(first, modes), :]

    def decode(t):
        slot, there = lax.rem(t, DONE_SLOTS), lax.rem(t, ARRIVED_SLOTS)

        def tile(index, carry):
            rows = pl.ds(pl.multiple_of(index * 32, 32), 32)
            high, low = split(arrived[there, rows, :])
            c_hi[rows, :] = high
            c_lo[rows, :] = low
            return carry

        lax.fori_loop(0, padded // 32, tile, 0)
        odd = dot3(fill_hi[...], fill_lo[...], c_hi[...], c_lo[...])
        for which in range(SIDE):
            done[slot, which, modes:] += odd[which * modes : (which + 1) * modes]

    for half in range(2):
        load(0, half).start()

    arrived[:, rank:padded] = jnp.zeros((arrived.shape[0], padded - rank, arrived.shape[2]), jnp.float32)
    barrier = pltpu.get_barrier_semaphore()
    for peer in (x_peer, z_peer):
        pl.semaphore_signal(
            barrier, inc=1, device_id={"lon": peer}, device_id_type=pl.DeviceIdType.MESH
        )

    @pl.when(inner)
    def _():
        pl.semaphore_signal(
            barrier, inc=1, device_id={"lon": m_peer}, device_id_type=pl.DeviceIdType.MESH
        )

    arrange(0)

    @pl.when(inner)
    def _():
        pl.semaphore_wait(barrier, 3)

    @pl.when(outer)
    def _():
        pl.semaphore_wait(barrier, 2)

    @pl.when(outer)
    def _():
        for part in range(SLABS):
            samples_z(0, x, row, part).start()

    for part in range(SLABS):
        samples_x(0, place, part).start()

    @pl.when(inner)
    def _():
        for copy in tables:
            copy.start()

    for half in range(2):
        load(1, half).start()

    for t in range(1, AHEAD):
        arrange(t)
        for part in range(SLABS):
            samples_x(t, place, part).start()

    def step(i, carry):
        @pl.when(outer & (i >= SENT_LAG) & (i < chunks + SENT_LAG))
        def _():
            for which in range(2):
                for part in range(SLABS):
                    samples_z(i - SENT_LAG, which, row, part).wait_send()

        @pl.when(i + AHEAD < chunks)
        def _():
            arrange(i + AHEAD)
            for part in range(SLABS):
                samples_x(i + AHEAD, place, part).start()

        @pl.when(outer & (i < chunks))
        def _():
            for part in range(SLABS):
                samples_x(i, beside, part).wait_recv()
                samples_z(i, 1 - x, row, part).start()

            @pl.when(i + 1 < chunks)
            def _():
                for part in range(SLABS):
                    samples_z(i + 1, x, row, part).start()

        @pl.when(outer & (i >= LAG) & (i < chunks + LAG))
        def _():
            t = i - LAG
            for part in range(2):
                modes_z(t, 1 - x, row, part).wait_recv()
                modes_x(t, part).start()
            for part in range(2):
                modes_z(t, x, row, part).wait_recv()
            store(t, x, done.at[lax.rem(t, DONE_SLOTS), place])

        @pl.when(outer & (i >= LAG + 1) & (i < chunks + LAG + 1))
        def _():
            t = i - LAG - 1
            for part in range(2):
                modes_x(t, part).wait_send()
                modes_x(t, part).wait_recv()
            store(t, 1 - x, cross.at[lax.rem(t, CROSS_SLOTS)])

        @pl.when(inner & (i < chunks))
        def _():
            for part in range(SLABS):
                samples_x(i, beside, part).wait_recv()
                for which in range(2):
                    samples_z(i, which, 1 - row, part).wait_recv()

            @pl.when(i == 0)
            def _():
                for copy in tables:
                    copy.wait()

            encode(i)
            own_modes(i)

        @pl.when(inner & (i >= 1) & (i < chunks + 1))
        def _():
            t = i - 1
            code(t, 0, 1 - row).wait_recv()
            add_evens(t, 1 - row)
            for which in (1 - x, x):
                modes_z(t, which, 1 - row, 0).start()
            code(t, 1, 1 - row).wait_recv()
            add_evens(t, row)
            modes_x(t, 0).start()
            decode(t)
            modes_z(t, 1 - x, 1 - row, 1).start()
            modes_x(t, 1).start()
            modes_z(t, x, 1 - row, 1).start()
            store(t, x, done.at[lax.rem(t, DONE_SLOTS), place])

        @pl.when(inner & (i >= 2) & (i < chunks + 2))
        def _():
            t = i - 2
            for part in range(2):
                modes_x(t, part).wait_recv()
            store(t, 1 - x, cross.at[lax.rem(t, CROSS_SLOTS)])

        return carry

    lax.fori_loop(0, chunks + LAG + 1, step, 0)

    for part in range(SLABS):
        for back in range(OTHER_SLOTS):
            samples_x(chunks - 1 - back, place, part).wait_send()

    @pl.when(inner)
    def _():
        for part in range(2):
            for back in range(CODED_SLOTS):
                code(chunks - 1 - back, part, row).wait_send()
            for back in range(DONE_SLOTS):
                for which in range(2):
                    modes_z(chunks - 1 - back, which, 1 - row, part).wait_send()
                modes_x(chunks - 1 - back, part).wait_send()


def fused_local(state):
    points, fields, lat_dev = state.shape
    modes = points // 2
    groups = fields // SUBLANES
    chunks = groups * PIECES
    tables = all_tables(points)
    padded = tables[2].shape[1]
    rank = RADIX * points // 4 + EXTRA
    vmem = pl.BlockSpec(memory_space=pltpu.VMEM)
    hbm = pl.BlockSpec(memory_space=pl.ANY)
    wide = FIELDS * LANES
    dma = pltpu.SemaphoreType.DMA

    def f32(*shape):
        return pltpu.VMEM(shape, jnp.float32)

    def bf16(*shape):
        return pltpu.VMEM(shape, jnp.bfloat16)

    result = pl.pallas_call(
        functools.partial(kernel, chunks, rank),
        out_shape=pltpu.VMEM((2, modes, groups, 2, SUBLANES, LANES), jnp.float32),
        in_specs=[hbm] * (1 + len(tables)),
        out_specs=vmem,
        scratch_shapes=[
            f32(2, 2, points, SUBLANES, LANES),
            f32(GRID_SLOTS, SIDE, points, wide),
            f32(OTHER_SLOTS, points, wide),
            f32(CODED_SLOTS, padded, wide),
            f32(ARRIVED_SLOTS, padded, wide),
            f32(DONE_SLOTS, SIDE, points, wide),
            f32(CROSS_SLOTS, points, wide),
            *[bf16(*table.shape[1:]) for table in tables],
            bf16(SIDE * points, wide),
            bf16(SIDE * points, wide),
            bf16(padded, wide),
            bf16(padded, wide),
            dma((2, 2)),
            dma((len(tables),)),
            dma((OTHER_SLOTS, SLABS)),
            dma((GRID_SLOTS, SLABS)),
            dma((GRID_SLOTS, 2, SLABS)),
            dma((GRID_SLOTS, 2, SLABS)),
            dma((CODED_SLOTS, 2)),
            dma((ARRIVED_SLOTS, 2)),
            dma((DONE_SLOTS, 2, 2)),
            dma((DONE_SLOTS, 2, 2)),
            dma((DONE_SLOTS, 2)),
            dma((CROSS_SLOTS, 2)),
        ],
        compiler_params=pltpu.CompilerParams(
            collective_id=0, has_side_effects=True, vmem_limit_bytes=VMEM_LIMIT
        ),
    )(state, *tables)
    return result.transpose(0, 1, 2, 4, 3, 5).reshape(2, modes, fields, lat_dev)


def solution(mesh):
    devices = mesh.shape["lon"]

    def local(state):
        points, fields, lat_dev = state.shape
        fits = (
            devices == RADIX
            and fields == RADIX * SUBLANES
            and points == 2 * LANES
            and lat_dev == 2 * LANES
        )
        return fused_local(state) if fits else dense_local(state)

    return jax.shard_map(
        local,
        mesh=mesh,
        in_specs=(P("lon", None, "lat"),),
        out_specs=P(None, "lon", None, "lat"),
        check_vma=False,
    )
```
